8 devices in a mesh: fsdp: 2 (over z, y), ep: 4 (over x, core).
Axes of the slice: x: 2, y: 2, z: 1, core: 2. Of those that a mesh axis runs over, the one named last changes fastest.
Arguments:
- x_tok: bfloat16 [32768, 896], P(('fsdp', 'ep'))
- dy_tok: bfloat16 [32768, 896], P(('fsdp', 'ep'))
- expert_idx: int32 [32768, 8], P(('fsdp', 'ep'))
- gate_val: float32 [32768, 8], P(('fsdp', 'ep'))
- w_one: bfloat16 [256, 896, 256], P('ep', 'fsdp')
- w_two: bfloat16 [256, 256, 896], P('ep', None, 'fsdp')
- w_three: bfloat16 [256, 896, 256], P('ep', 'fsdp')
- ws_one: bfloat16 [896, 256], P('fsdp')
- ws_two: bfloat16 [256, 896], P(None, 'fsdp')
- ws_three: bfloat16 [896, 256], P('fsdp')
Outputs:
- output 1: bfloat16 [32768, 896], P(('fsdp', 'ep'))
- output 2: float32 [32768, 8], P(('fsdp', 'ep'))
- output 3: float32 [256, 896, 256], P('ep', 'fsdp')
- output 4: float32 [256, 256, 896], P('ep', None, 'fsdp')
- output 5: float32 [256, 896, 256], P('ep', 'fsdp')
- output 6: float32 [896, 256], P('fsdp')
- output 7: float32 [256, 896], P(None, 'fsdp')
- output 8: float32 [896, 256], P('fsdp')
All inputs are finite; a program needn't handle non-finite values.
Results may differ from the reference program's by a relative error of at most 0.00489957.
Values are sent between devices in bfloat16 or wider.
A program may use at most 1 GiB of HBM per device.

```python
import jax
import jax.numpy as jnp
from jax import lax

MODEL_DIM = 896
EXPERT_FF = 256
SHARED_FF = 256
EXPERTS = 256
TOP_K = 8
TOK_DEV = 4096
SRC_DEVICES = 8
CAPACITY = 160

TOKENS = TOK_DEV * SRC_DEVICES


def draw_routing(key):
    key_list = jax.random.split(key, 5)
    spread = EXPERTS // TOP_K
    jitter = max(spread // 4, 1)
    hot_span = max(EXPERTS // 8, 1)
    hot_start = jax.random.randint(key_list[0], (), 0, EXPERTS)
    is_hot = jax.random.randint(key_list[1], (TOKENS, 1), 0, 4) == 0
    base_hot = hot_start + jax.random.randint(key_list[2], (TOKENS, 1), 0, hot_span)
    base_any = jax.random.randint(key_list[3], (TOKENS, 1), 0, EXPERTS)
    base_id = jnp.where(is_hot, base_hot, base_any)
    offsets = jnp.arange(TOP_K, dtype=jnp.int32)[None, :] * spread + jax.random.randint(key_list[4], (TOKENS, TOP_K), 0, jitter)
    return ((base_id + offsets) % EXPERTS).astype(jnp.int32)


def setup_inputs(seed: int = 0) -> dict:
    key_list = jax.random.split(jax.random.key(seed), 10)
    dim_scale = MODEL_DIM ** -0.5
    ff_scale = EXPERT_FF ** -0.5
    shared_scale = SHARED_FF ** -0.5
    x_tok = jax.random.normal(key_list[0], (TOKENS, MODEL_DIM), jnp.float32).astype(jnp.bfloat16)
    dy_tok = jax.random.normal(key_list[1], (TOKENS, MODEL_DIM), jnp.float32).astype(jnp.bfloat16)
    expert_idx = draw_routing(key_list[2])
    gate_val = jax.random.uniform(key_list[3], (TOKENS, TOP_K), jnp.float32, 0.3, 1.0)
    w_one = (jax.random.normal(key_list[4], (EXPERTS, MODEL_DIM, EXPERT_FF), jnp.float32) * dim_scale).astype(jnp.bfloat16)
    w_two = (jax.random.normal(key_list[5], (EXPERTS, EXPERT_FF, MODEL_DIM), jnp.float32) * ff_scale).astype(jnp.bfloat16)
    w_three = (jax.random.normal(key_list[6], (EXPERTS, MODEL_DIM, EXPERT_FF), jnp.float32) * dim_scale).astype(jnp.bfloat16)
    ws_one = (jax.random.normal(key_list[7], (MODEL_DIM, SHARED_FF), jnp.float32) * dim_scale).astype(jnp.bfloat16)
    ws_two = (jax.random.normal(key_list[8], (SHARED_FF, MODEL_DIM), jnp.float32) * shared_scale).astype(jnp.bfloat16)
    ws_three = (jax.random.normal(key_list[9], (MODEL_DIM, SHARED_FF), jnp.float32) * dim_scale).astype(jnp.bfloat16)
    return {"x_tok": x_tok, "dy_tok": dy_tok, "expert_idx": expert_idx, "gate_val": gate_val, "w_one": w_one, "w_two": w_two, "w_three": w_three, "ws_one": ws_one, "ws_two": ws_two, "ws_three": ws_three}


def slots_for_source(ids_src):
    flat_ids = ids_src.reshape(-1)
    onehot = (flat_ids[:, None] == jnp.arange(EXPERTS, dtype=jnp.int32)[None, :]).astype(jnp.int32)
    slot_pos = jnp.sum(jnp.cumsum(onehot, axis=0) * onehot, axis=1) - 1
    return jnp.where(slot_pos < CAPACITY, flat_ids * CAPACITY + slot_pos, EXPERTS * CAPACITY)


def fill_for_source(slot_idx):
    n_assign = TOK_DEV * TOP_K
    filled = jnp.full((EXPERTS * CAPACITY + 1,), n_assign, jnp.int32)
    filled = filled.at[slot_idx].set(jnp.arange(n_assign, dtype=jnp.int32))
    return filled[: EXPERTS * CAPACITY]


def swiglu_grads(x_rows, g_rows, w_a, w_b, w_c):
    h_one = jnp.dot(x_rows, w_a, preferred_element_type=jnp.float32)
    h_three = jnp.dot(x_rows, w_c, preferred_element_type=jnp.float32)
    sig_one = jax.nn.sigmoid(h_one)
    silu_one = h_one * sig_one
    act_rows = (silu_one * h_three).astype(jnp.bfloat16)
    d_act = jnp.dot(g_rows, w_b.T, preferred_element_type=jnp.float32)
    dh_one = (d_act * h_three * sig_one * (1.0 + h_one * (1.0 - sig_one))).astype(jnp.bfloat16)
    dh_three = (d_act * silu_one).astype(jnp.bfloat16)
    dx_rows = (jnp.dot(dh_one, w_a.T, preferred_element_type=jnp.float32) + jnp.dot(dh_three, w_c.T, preferred_element_type=jnp.float32)).astype(jnp.bfloat16)
    dw_a = jnp.dot(x_rows.T, dh_one, preferred_element_type=jnp.float32)
    dw_b = jnp.dot(act_rows.T, g_rows, preferred_element_type=jnp.float32)
    dw_c = jnp.dot(x_rows.T, dh_three, preferred_element_type=jnp.float32)
    return dx_rows, act_rows, dw_a, dw_b, dw_c


def reference(x_tok, dy_tok, expert_idx, gate_val, w_one, w_two, w_three, ws_one, ws_two, ws_three):
    n_assign = TOK_DEV * TOP_K
    slot_idx = jax.vmap(slots_for_source)(expert_idx.reshape(SRC_DEVICES, TOK_DEV, TOP_K))
    filled = jax.vmap(fill_for_source)(slot_idx)
    src_base = jnp.arange(SRC_DEVICES, dtype=jnp.int32)[:, None] * n_assign
    global_ids = jnp.where(filled < n_assign, filled + src_base, TOKENS * TOP_K)
    expert_rows = global_ids.reshape(SRC_DEVICES, EXPERTS, CAPACITY).transpose(1, 0, 2).reshape(EXPERTS, SRC_DEVICES * CAPACITY)
    zero_row = jnp.zeros((1, MODEL_DIM), jnp.bfloat16)
    x_pad = jnp.concatenate([x_tok, zero_row])
    dy_pad = jnp.concatenate([dy_tok, zero_row])
    gate_pad = jnp.concatenate([gate_val.reshape(-1), jnp.zeros((1,), jnp.float32)])

    def expert_step(acc_state, step_in):
        dx_acc, dgate_acc = acc_state
        assign_ids, w_a, w_b, w_c = step_in
        tok_ids = assign_ids // TOP_K
        x_rows = x_pad[tok_ids]
        dy_rows = dy_pad[tok_ids]
        dy_wide = dy_rows.astype(jnp.float32)
        g_rows = (gate_pad[assign_ids][:, None] * dy_wide).astype(jnp.bfloat16)
        dx_rows, act_rows, dw_a, dw_b, dw_c = swiglu_grads(x_rows, g_rows, w_a, w_b, w_c)
        y_rows = jnp.dot(act_rows, w_b, preferred_element_type=jnp.float32)
        dgate_rows = jnp.sum(dy_wide * y_rows, axis=1)
        dx_acc = dx_acc.at[tok_ids].add(dx_rows.astype(jnp.float32))
        dgate_acc = dgate_acc.at[assign_ids].add(dgate_rows)
        return (dx_acc, dgate_acc), (dw_a, dw_b, dw_c)

    init_state = (jnp.zeros((TOKENS + 1, MODEL_DIM), jnp.float32), jnp.zeros((TOKENS * TOP_K + 1,), jnp.float32))
    final_state, expert_grads = lax.scan(expert_step, init_state, (expert_rows, w_one, w_two, w_three))

    def shared_step(acc_state, step_in):
        x_rows, dy_rows = step_in
        dx_rows, act_rows, dw_a, dw_b, dw_c = swiglu_grads(x_rows, dy_rows, ws_one, ws_two, ws_three)
        return (acc_state[0] + dw_a, acc_state[1] + dw_b, acc_state[2] + dw_c), dx_rows

    shared_init = (jnp.zeros((MODEL_DIM, SHARED_FF), jnp.float32), jnp.zeros((SHARED_FF, MODEL_DIM), jnp.float32), jnp.zeros((MODEL_DIM, SHARED_FF), jnp.float32))
    x_blocks = x_tok.reshape(SRC_DEVICES, TOK_DEV, MODEL_DIM)
    dy_blocks = dy_tok.reshape(SRC_DEVICES, TOK_DEV, MODEL_DIM)
    shared_grads, dx_shared = lax.scan(shared_step, shared_init, (x_blocks, dy_blocks))
    dx_acc, dgate_acc = final_state
    dx_out = (dx_acc[:TOKENS] + dx_shared.reshape(TOKENS, MODEL_DIM).astype(jnp.float32)).astype(jnp.bfloat16)
    dgate = dgate_acc[: TOKENS * TOP_K].reshape(TOKENS, TOP_K)
    return (dx_out, dgate, expert_grads[0], expert_grads[1], expert_grads[2], shared_grads[0], shared_grads[1], shared_grads[2])
```

```python
import functools
import jax
import jax.numpy as jnp
from jax import lax
from jax.experimental import pallas as pl
from jax.experimental.pallas import tpu as pltpu
from jax.sharding import PartitionSpec as P


BF = jnp.bfloat16
F32 = jnp.float32
LANE = 128
SUB = 8
CAP_NUM = 5
CAP_DEN = 4
N_GROUP = 8


def capacity_for(tok_dev, top_k, n_exp):
    needed = -(-(tok_dev * top_k * CAP_NUM) // (CAP_DEN * n_exp))
    return max(8, -(-needed // 8) * 8)


def gather_kernel(own, cap, chunk, start_ref, cnt_ref, tok_ref, gate_ref, x_hbm, d_hbm, *rest):
    n_out = 3 if own else 2
    outs = rest[-7 - n_out:-7]
    xtab, dtab, xtile, gtile, dtile, stage, sem = rest[-7:]
    tok_dev, width = x_hbm.shape
    n_col = width // LANE
    e = pl.program_id(0)
    n_chunk = tok_dev // chunk

    def copies(c, slot):
        rows = pl.ds(c * chunk, chunk)
        return (
            pltpu.make_async_copy(x_hbm.at[rows, :], stage.at[slot, 0], sem.at[slot, 0]),
            pltpu.make_async_copy(d_hbm.at[rows, :], stage.at[slot, 1], sem.at[slot, 1]),
        )

    @pl.when(e == 0)
    def _():
        for cp in copies(0, 0):
            cp.start()

        @pl.loop(0, n_chunk)
        def _(c):
            slot = lax.rem(c, 2)

            @pl.when(c + 1 < n_chunk)
            def _():
                for cp in copies(c + 1, 1 - slot):
                    cp.start()

            for cp in copies(c, slot):
                cp.wait()
            for which, tab in ((0, xtab), (1, dtab)):
                @pl.loop(0, chunk // 16)
                def _(r):
                    rows = stage[slot, which, pl.ds(pl.multiple_of(r * 16, 16), 16), :].astype(F32)
                    for half in range(2):
                        base = (c * chunk + r * 16 + half * SUB) * SUB
                        for j in range(n_col):
                            tab[pl.ds(base + j, SUB, stride=SUB), :] = rows[half * SUB:(half + 1) * SUB, j * LANE:(j + 1) * LANE]

    s0 = start_ref[e]
    n = cnt_ref[e]
    unroll = 16

    @pl.loop(0, pl.cdiv(n, unroll))
    def _(b):
        first = s0 + b * unroll
        for i in range(unroll):
            row = pl.multiple_of(tok_ref[first + i], SUB)
            gate = gate_ref[first + i]
            dst = pl.ds(pl.multiple_of((b * unroll + i) * SUB, SUB), SUB)
            xtile[dst, :] = xtab[pl.ds(row, SUB), :]
            drow = dtab[pl.ds(row, SUB), :]
            gtile[dst, :] = drow * gate
            if own:
                dtile[dst, :] = drow

    tiles = (xtile, gtile, dtile) if own else (xtile, gtile)
    for tile, out in zip(tiles, outs):
        @pl.loop(0, cap // 16)
        def _(r):
            pos = lax.broadcasted_iota(jnp.int32, (16, LANE), 0) + r * 16
            keep = pos < n
            for j in range(n_col):
                lo = tile[pl.ds(r * 16 * SUB + j, SUB, stride=SUB), :]
                hi = tile[pl.ds(r * 16 * SUB + SUB * SUB + j, SUB, stride=SUB), :]
                both = jnp.concatenate([lo, hi], axis=0)
                both = jnp.where(keep, both, 0.0).astype(BF)
                out[0, 0, pl.ds(pl.multiple_of(r * 16, 16), 16), j * LANE:(j + 1) * LANE] = both


def gather_call(plane, bufs, starts, counts, tok8, gates, x_loc, d_loc, n_src, cap, own):
    n_local = starts.shape[0]
    tok_dev, width = x_loc.shape
    chunk = min(512, tok_dev)
    smem = pl.BlockSpec(memory_space=pltpu.SMEM)
    anyspec = pl.BlockSpec(memory_space=pl.ANY)
    n_buf = 3 if own else 2
    shapes = [jax.ShapeDtypeStruct((n_local, n_src if i < 2 else n_src // 2, cap, width), BF) for i in range(n_buf)]
    out_specs = [pl.BlockSpec((1, 1, cap, width), lambda e: (e, plane, 0, 0)) for _ in range(n_buf)]
    scratch = [
        pltpu.VMEM((tok_dev * SUB, LANE), F32),
        pltpu.VMEM((tok_dev * SUB, LANE), F32),
        pltpu.VMEM((cap * SUB, LANE), F32),
        pltpu.VMEM((cap * SUB, LANE), F32),
        pltpu.VMEM((cap * SUB if own else SUB, LANE), F32),
        pltpu.VMEM((2, 2, chunk, width), BF),
        pltpu.SemaphoreType.DMA((2, 2)),
    ]
    args = [starts, counts, tok8, gates, x_loc, d_loc]
    return pl.pallas_call(
        functools.partial(gather_kernel, own, cap, chunk),
        grid=(n_local,),
        in_specs=[smem, smem, smem, smem, anyspec, anyspec] + [anyspec] * len(bufs),
        out_specs=out_specs,
        out_shape=shapes,
        scratch_shapes=scratch,
        input_output_aliases={6 + i: i for i in range(len(bufs))},
        compiler_params=pltpu.CompilerParams(vmem_limit_bytes=60 * 1024 * 1024),
        name="gather_own" if own else "gather_other",
        cost_estimate=pl.CostEstimate(flops=30_000_000_000, bytes_accessed=60_000_000, transcendentals=0),
    )(*args, *bufs)


def _dot(a, b):
    return jnp.dot(a, b, preferred_element_type=F32)


def _dot_t(a, b):
    return lax.dot_general(a, b, (((1,), (1,)), ((), ())), preferred_element_type=F32)


def _dot_tn(a, b):
    return lax.dot_general(a, b, (((0,), (0,)), ((), ())), preferred_element_type=F32)


def expert_kernel(n_dst, cap, half_ref, xs, gs, ds, w1, w3, w2, *rest):
    dx_outs = rest[:n_dst]
    dg_out, dw1_out, dw2_out, dw3_out, a_scr, dh_scr = rest[n_dst:]
    n_own = n_dst * cap
    rows_all, width = xs.shape[1], xs.shape[2]
    ff = w1.shape[2]
    mine = width // 2
    half = half_ref[0]
    lo = (mine // LANE) * LANE
    wide = width - lo
    off = mine - lo
    for blk in range(rows_all // n_own):
        rows = slice(blk * n_own, (blk + 1) * n_own)
        x = xs[0, rows, :]
        h1 = _dot(x, w1[0])
        h3 = _dot(x, w3[0])
        da = _dot(gs[0, rows, :], w2[0])
        sig = jax.nn.sigmoid(h1)
        silu = h1 * sig
        a_scr[rows, :] = (silu * h3).astype(BF)
        dh_scr[rows, :ff] = (da * h3 * sig * (1.0 + h1 * (1.0 - sig))).astype(BF)
        dh_scr[rows, ff:] = (da * silu).astype(BF)
        if blk == 0:
            dx = _dot_t(dh_scr[rows, :ff], w1[0]) + _dot_t(dh_scr[rows, ff:], w3[0])
            dxb = dx.astype(BF)
            for s in range(n_dst):
                dx_outs[s][0] = dxb[s * cap:(s + 1) * cap, :]
            prod = _dot_t(a_scr[rows, :], w2[0]) * ds[0].astype(F32)
            part = prod[:, :LANE]
            for j in range(1, width // LANE):
                part = part + prod[:, j * LANE:(j + 1) * LANE]
            for r in range(n_own // LANE):
                dg_out[0, :, r * LANE:(r + 1) * LANE] = jnp.sum(part[r * LANE:(r + 1) * LANE, :].T, axis=0, keepdims=True)
    start = pl.multiple_of(half * lo, LANE)
    xh = xs[0, :, pl.ds(start, wide)]
    gh = gs[0, :, pl.ds(start, wide)]
    dw13 = _dot_tn(xh, dh_scr[...])
    dw2 = _dot_tn(gh, a_scr[...])

    @pl.when(half == 0)
    def _():
        dw1_out[0] = dw13[:mine, :ff]
        dw3_out[0] = dw13[:mine, ff:]
        dw2_out[0] = dw2[:mine, :]

    @pl.when(half != 0)
    def _():
        dw1_out[0] = dw13[off:, :ff]
        dw3_out[0] = dw13[off:, ff:]
        dw2_out[0] = dw2[off:, :]


def expert_call(half, xs, gs, ds, w_all, base, bufs):
    n_grp, width, ff = w_all.shape[0] // 3, w_all.shape[1], w_all.shape[2]
    n_local, n_src, cap = xs.shape[:3]
    n_own = ds.shape[1]
    mine = width // 2
    xs = xs.reshape(n_local, n_src * cap, width)
    gs = gs.reshape(n_local, n_src * cap, width)
    ds = ds.reshape(n_local, n_own * cap, width)
    at = lambda e: (e + base, 0, 0)
    loc = lambda e: (e, 0, 0)
    in_specs = [
        pl.BlockSpec(memory_space=pltpu.SMEM),
        pl.BlockSpec((1, n_src * cap, width), at),
        pl.BlockSpec((1, n_src * cap, width), at),
        pl.BlockSpec((1, n_own * cap, width), at),
        pl.BlockSpec((1, width, ff), loc),
        pl.BlockSpec((1, width, ff), lambda e: (e + n_grp, 0, 0)),
        pl.BlockSpec((1, width, ff), lambda e: (e + 2 * n_grp, 0, 0)),
    ]
    out_specs = [pl.BlockSpec((1, cap, width), loc)] * n_own
    out_specs += [pl.BlockSpec((1, 1, n_own * cap), loc)] + [pl.BlockSpec((1, mine, ff), at)] * 3
    out_shape = [jax.ShapeDtypeStruct((n_grp, cap, width), BF)] * n_own
    out_shape += [jax.ShapeDtypeStruct((n_grp, 1, n_own * cap), F32)] + [jax.ShapeDtypeStruct((n_local, mine, ff), F32)] * 3
    args = [half, xs, gs, ds, w_all, w_all, w_all]
    n_alias = 0 if bufs is None else 3
    if bufs is not None:
        in_specs += [pl.BlockSpec(memory_space=pl.ANY)] * 3
        args += list(bufs)

    def body(*refs):
        expert_kernel(n_own, cap, *refs[:7], *refs[7 + n_alias:])

    flops = 2 * n_grp * width * ff * (3 * n_src * cap + 3 * n_own * cap + 3 * n_src * cap // 2)
    outs = pl.pallas_call(
        body,
        grid=(n_grp,),
        in_specs=in_specs,
        out_specs=out_specs,
        out_shape=out_shape,
        scratch_shapes=[pltpu.VMEM((n_src * cap, ff), BF), pltpu.VMEM((n_src * cap, 2 * ff), BF)],
        input_output_aliases={7 + i: n_own + 1 + i for i in range(n_alias)},
        compiler_params=pltpu.CompilerParams(vmem_limit_bytes=60 * 1024 * 1024),
        name="experts",
        cost_estimate=pl.CostEstimate(flops=flops, bytes_accessed=n_grp * 9_000_000, transcendentals=n_grp * n_src * cap * ff),
    )(*args)
    return outs[:n_own], outs[n_own], outs[n_own + 1:]


def combine_kernel(n_ep, base, first, last, n_rows, *refs):
    me_ref, start_ref, cnt_ref, asg_ref, dg_ref = refs[:5]
    rest = refs[5:]
    rows_hbm, rest = rest[:n_rows], rest[n_rows:]
    if not first:
        acc_in, rest = rest[0], rest[1:]
    if last:
        shared_ref, rest = rest[0], rest[1:]
        dx_out, dg_out, rest = rest[0], rest[1], rest[2:]
    else:
        acc_out, rest = rest[0], rest[1:]
    acc, tile, buf, sem, acc_sem = rest
    n_grp, cap, width = rows_hbm[0].shape
    n_col = width // LANE
    pitch = cap + SUB
    n_exp = start_ref.shape[0]
    n_local = n_exp // n_ep
    tok_rows = acc.shape[0]
    per = n_rows // n_ep * n_grp

    def fetch(i, slot, go):
        for k in range(n_rows):
            @pl.when(lax.div(i, n_grp) == k)
            def _():
                cp = pltpu.make_async_copy(rows_hbm[k].at[lax.rem(i, n_grp)], buf.at[slot], sem.at[slot])
                cp.start() if go else cp.wait()

    fetch(0, 0, True)
    if first:
        @pl.loop(0, tok_rows // 64)
        def _(r):
            acc[pl.ds(pl.multiple_of(r * 64, 64), 64), :] = jnp.zeros((64, LANE), F32)
    else:
        pltpu.make_async_copy(acc_in, acc, acc_sem).start()
        pltpu.make_async_copy(acc_in, acc, acc_sem).wait()
    tile[n_col * pitch:, :] = jnp.zeros((tile.shape[0] - n_col * pitch, LANE), F32)
    code = jnp.where(
        lax.broadcasted_iota(jnp.int32, (SUB, LANE), 0) == n_col,
        lax.broadcasted_iota(jnp.int32, (SUB, LANE), 1),
        -1,
    )

    @pl.loop(0, n_rows * n_grp)
    def _(i):
        slot = lax.rem(i, 2)

        @pl.when(i + 1 < n_rows * n_grp)
        def _():
            fetch(i + 1, 1 - slot, True)

        fetch(i, slot, False)
        e = jnp.bitwise_xor(me_ref[1], lax.div(i, per)) * n_local + base + lax.rem(i, per)

        @pl.loop(0, cap // 16)
        def _(r):
            for j in range(n_col):
                v = buf[slot, pl.ds(pl.multiple_of(r * 16, 16), 16), j * LANE:(j + 1) * LANE].astype(F32)
                tile[pl.ds(pl.multiple_of(j * pitch + r * 16, SUB), 16), :] = v

        s0 = start_ref[e]
        d0 = i * cap
        unroll = 16

        @pl.loop(0, pl.cdiv(cnt_ref[e], unroll))
        def _(b):
            pos = b * unroll
            for u in range(unroll):
                a = asg_ref[s0 + pos + u]
                row = tile[pl.ds(pos + u, SUB, stride=pitch), :]
                row = jnp.where(code == (a & (SUB - 1)), dg_ref[d0 + pos + u], row)
                dst = pl.ds(pl.multiple_of(a & -SUB, SUB), SUB)
                acc[dst, :] = acc[dst, :] + row

    if last:
        @pl.loop(0, tok_rows // (16 * SUB))
        def _(r):
            rows = pl.ds(pl.multiple_of(r * 16, 16), 16)
            both = []
            for j in range(n_col + 1):
                lo = acc[pl.ds(r * 16 * SUB + j, SUB, stride=SUB), :]
                hi = acc[pl.ds(r * 16 * SUB + SUB * SUB + j, SUB, stride=SUB), :]
                both.append(jnp.concatenate([lo, hi], axis=0))
            for j in range(n_col):
                col = slice(j * LANE, (j + 1) * LANE)
                dx_out[rows, col] = (both[j] + shared_ref[rows, col].astype(F32)).astype(BF)
            dg_out[rows, :] = both[n_col]
    else:
        pltpu.make_async_copy(acc, acc_out, acc_sem).start()
        pltpu.make_async_copy(acc, acc_out, acc_sem).wait()


def combine_call(place, starts, counts, asg, dg, rows, base, acc, shared, n_ep, tok_dev):
    n_rows = len(rows)
    first, last = acc is None, shared is not None
    _, cap, width = rows[0].shape
    smem = pl.BlockSpec(memory_space=pltpu.SMEM)
    anyspec = pl.BlockSpec(memory_space=pl.ANY)
    vmem = pl.BlockSpec(memory_space=pltpu.VMEM)
    args = [place, starts, counts, asg, dg, *rows]
    in_specs = [smem] * 5 + [anyspec] * n_rows
    if not first:
        args.append(acc)
        in_specs.append(anyspec)
    if last:
        args.append(shared)
        in_specs.append(vmem)
        out_shape = [jax.ShapeDtypeStruct((tok_dev, width), BF), jax.ShapeDtypeStruct((tok_dev, LANE), F32)]
        out_specs = [vmem, vmem]
    else:
        out_shape = jax.ShapeDtypeStruct((tok_dev * SUB, LANE), F32)
        out_specs = anyspec
    return pl.pallas_call(
        functools.partial(combine_kernel, n_ep, base, first, last, n_rows),
        in_specs=in_specs,
        out_specs=out_specs,
        out_shape=out_shape,
        scratch_shapes=[
            pltpu.VMEM((tok_dev * SUB, LANE), F32),
            pltpu.VMEM((SUB * (cap + SUB), LANE), F32),
            pltpu.VMEM((2, cap, width), BF),
            pltpu.SemaphoreType.DMA((2,)),
            pltpu.SemaphoreType.DMA,
        ],
        input_output_aliases={} if first or last else {5 + n_rows: 0},
        compiler_params=pltpu.CompilerParams(vmem_limit_bytes=60 * 1024 * 1024),
        name="combine",
        cost_estimate=pl.CostEstimate(flops=n_rows * 3_000_000_000, bytes_accessed=n_rows * 3_000_000, transcendentals=0),
    )(*args)


def sort_assignments(ids_dev, gate_dev, n_exp, cap):
    n_assign = ids_dev.size
    key = ids_dev.reshape(-1) * n_assign + jnp.arange(n_assign, dtype=jnp.int32)
    key, gates = lax.sort((key, gate_dev.reshape(-1)), num_keys=1)
    edges = jnp.arange(n_exp + 1, dtype=jnp.int32) * n_assign
    starts = jnp.sum((key[None, :] < edges[:, None]).astype(jnp.int32), axis=1)
    counts = jnp.minimum(starts[1:] - starts[:-1], cap)
    pad = 2 * LANE
    asg = jnp.pad(key & (n_assign - 1), (0, pad))
    return asg, jnp.pad(gates, (0, pad)), starts[:-1], counts


def shared_backward(x_rows, g_rows, w_a, w_b, w_c):
    h_one = _dot(x_rows, w_a)
    h_three = _dot(x_rows, w_c)
    sig_one = jax.nn.sigmoid(h_one)
    silu_one = h_one * sig_one
    act_rows = (silu_one * h_three).astype(BF)
    d_act = _dot_t(g_rows, w_b)
    dh_one = (d_act * h_three * sig_one * (1.0 + h_one * (1.0 - sig_one))).astype(BF)
    dh_three = (d_act * silu_one).astype(BF)
    dx_rows = (_dot_t(dh_one, w_a) + _dot_t(dh_three, w_c)).astype(BF)
    return dx_rows, _dot_tn(x_rows, dh_one), _dot_tn(act_rows, g_rows), _dot_tn(x_rows, dh_three)


def solution(mesh):
    ep_size = mesh.shape["ep"]
    rows_size = mesh.shape["fsdp"]
    tok_spec = P(("fsdp", "ep"), None)
    in_specs = (tok_spec, tok_spec, tok_spec, tok_spec, P("ep", "fsdp", None), P("ep", None, "fsdp"), P("ep", "fsdp", None), P("fsdp", None), P(None, "fsdp"), P("fsdp", None))
    out_specs = (tok_spec, tok_spec, P("ep", "fsdp", None), P("ep", None, "fsdp"), P("ep", "fsdp", None), P("fsdp", None), P(None, "fsdp"), P("fsdp", None))

    def swap_row(v):
        return lax.ppermute(v, "fsdp", [(i, rows_size - 1 - i) for i in range(rows_size)])

    def swap_ep(v, k):
        return lax.ppermute(v, "ep", [(i, i ^ k) for i in range(ep_size)])

    def device_step(x_loc, dy_loc, ids_loc, gate_loc, w_one, w_two, w_three, ws_one, ws_two, ws_three):
        tok_dev, top_k = ids_loc.shape
        n_local = w_one.shape[0]
        n_exp = n_local * ep_size
        n_src = ep_size * rows_size
        cap = capacity_for(tok_dev, top_k, n_exp)
        n_grp = max(1, n_local // N_GROUP)
        n_parts = n_local // n_grp
        me, row = lax.axis_index("ep"), lax.axis_index("fsdp")
        place = jnp.stack([row, me]).astype(jnp.int32)

        near = (x_loc, dy_loc)
        far = tuple(swap_row(v) for v in near)
        near_x = tuple(swap_ep(v, 2) for v in near)
        near_c = tuple(swap_ep(v, 1) for v in near)

        ws_one_full = lax.all_gather(ws_one, "fsdp", axis=0, tiled=True)
        ws_three_full = lax.all_gather(ws_three, "fsdp", axis=0, tiled=True)
        ws_two_full = lax.all_gather(ws_two, "fsdp", axis=1, tiled=True)
        shared = shared_backward(x_loc, dy_loc, ws_one_full, ws_two_full, ws_three_full)
        dws_one = lax.psum(lax.psum_scatter(shared[1], "fsdp", scatter_dimension=0, tiled=True), "ep")
        dws_two = lax.psum(lax.psum_scatter(shared[2], "fsdp", scatter_dimension=1, tiled=True), "ep")
        dws_three = lax.psum(lax.psum_scatter(shared[3], "fsdp", scatter_dimension=0, tiled=True), "ep")

        ids_loc, gate_loc, shared = lax.optimization_barrier((ids_loc, gate_loc, shared))
        asg, gates, starts, counts = sort_assignments(ids_loc, gate_loc, n_exp, cap)
        n_list = asg.shape[0]
        meta = jnp.concatenate([asg & -SUB, starts, counts])
        meta_all = lax.all_gather(meta, ("fsdp", "ep"), axis=0)
        gates_all = lax.all_gather(gates, ("fsdp", "ep"), axis=0)

        def gather(plane, bufs, x_src, dy_src):
            own = plane < ep_size
            if plane == 0:
                meta_s, gates_s = meta, gates
            else:
                src = jnp.bitwise_xor(me, plane % ep_size) + ep_size * (row if own else rows_size - 1 - row)
                meta_s = lax.dynamic_index_in_dim(meta_all, src, 0, keepdims=False)
                gates_s = lax.dynamic_index_in_dim(gates_all, src, 0, keepdims=False)
            starts_s = lax.dynamic_slice(meta_s, (n_list + me * n_local,), (n_local,))
            counts_s = lax.dynamic_slice(meta_s, (n_list + n_exp + me * n_local,), (n_local,))
            take = tuple(bufs) if own else tuple(bufs[:2])
            new = gather_call(plane, take, starts_s, counts_s, meta_s[:n_list], gates_s, x_src, dy_src, n_src, cap, own)
            return tuple(new) + tuple(bufs[len(new):])

        bufs = gather(0, (), *near)
        bufs = gather(1, bufs, *near_c)

        sums = (dws_one, dws_two, dws_three)
        w_one, w_two, w_three, far, bufs, sums = lax.optimization_barrier((w_one, w_two, w_three, far, bufs, sums))
        dws_one, dws_two, dws_three = sums
        w_two = jnp.swapaxes(w_two, 1, 2)
        w_grp = []
        for g in range(n_parts):
            part = slice(g * n_grp, (g + 1) * n_grp)
            w_grp.append(lax.all_gather(jnp.concatenate([w_one[part], w_three[part], w_two[part]]), "fsdp", axis=1, tiled=True))
        far_x = tuple(swap_ep(v, 2) for v in far)
        far_c = tuple(swap_ep(v, 1) for v in far)
        near_xc = tuple(swap_ep(v, 1) for v in near_x)
        far_xc = tuple(swap_ep(v, 1) for v in far_x)
        for plane, src in enumerate((near_x, near_xc, far, far_c, far_x, far_xc), 2):
            order = plane if plane < ep_size else (4, 5, 6, 7)[plane - ep_size]
            bufs = gather(order, bufs, *src)
        xs, gs, ds = bufs

        grads = None
        back_rows, part_dg = [], []
        for g, w_full in enumerate(w_grp):
            dx_g, dg_g, grads = expert_call(place, xs, gs, ds, w_full, g * n_grp, grads)
            back_rows.append([dx_g[0]] + [swap_ep(dx_g[k], k) for k in range(1, ep_size)])
            part_dg.append(dg_g.reshape(n_grp, ep_size, cap))

        acc = None
        cuts = sorted({0, 5 * n_parts // 8, 7 * n_parts // 8, n_parts})
        for lo, hi in zip(cuts[:-1], cuts[1:]):
            dg = jnp.concatenate(part_dg[lo:hi])
            dg = [dg[:, 0]] + [swap_ep(dg[:, k], k) for k in range(1, ep_size)]
            dg = jnp.concatenate([d.reshape(-1) for d in dg])
            rows = [back_rows[g][k] for k in range(ep_size) for g in range(lo, hi)]
            final = shared[0] if hi == n_parts else None
            acc = combine_call(place, starts, counts, asg, dg, rows, lo * n_grp, acc, final, ep_size, tok_dev)
        dx_loc, dg_tok = acc
        dw_one, dw_two, dw_three = grads
        return dx_loc, dg_tok[:, :top_k], dw_one, jnp.swapaxes(dw_two, 1, 2), dw_three, dws_one, dws_two, dws_three

    return jax.shard_map(device_step, mesh=mesh, in_specs=in_specs, out_specs=out_specs, check_vma=False)
```

```python
import functools
import jax
import jax.numpy as jnp
from jax import lax
from jax.experimental import pallas as pl
from jax.experimental.pallas import tpu as pltpu
from jax.sharding import PartitionSpec as P


CAP_NUM = 5
CAP_DEN = 4
N_GROUP = 8
BF = jnp.bfloat16
F32 = jnp.float32
LANE = 128
SUB = 8
VMEM_LIMIT = 60 * 1024 * 1024


def capacity_for(tok_dev, top_k, n_exp):
    needed = -(-(tok_dev * top_k * CAP_NUM) // (CAP_DEN * n_exp))
    return max(8, -(-needed // 8) * 8)


def pitch_for(cap):
    return cap + 4


def gather_kernel(own, cap, chunk, start_ref, cnt_ref, tok_ref, gate_ref, x_hbm, d_hbm, *rest):
    n_out = 3 if own else 2
    outs = rest[-7 - n_out:-7]
    xtab, dtab, xtile, gtile, dtile, stage, sem = rest[-7:]
    tok_dev, width = x_hbm.shape
    n_col = width // LANE
    pitch = pitch_for(cap)
    e = pl.program_id(0)
    n_chunk = tok_dev // chunk

    def copies(c, slot):
        rows = pl.ds(c * chunk, chunk)
        return (
            pltpu.make_async_copy(x_hbm.at[rows, :], stage.at[slot, 0], sem.at[slot, 0]),
            pltpu.make_async_copy(d_hbm.at[rows, :], stage.at[slot, 1], sem.at[slot, 1]),
        )

    @pl.when(e == 0)
    def _():
        for cp in copies(0, 0):
            cp.start()

        @pl.loop(0, n_chunk)
        def _(c):
            slot = lax.rem(c, 2)

            @pl.when(c + 1 < n_chunk)
            def _():
                for cp in copies(c + 1, 1 - slot):
                    cp.start()

            for cp in copies(c, slot):
                cp.wait()

            @pl.loop(0, chunk // 16)
            def _(r):
                for which, tab in ((0, xtab), (1, dtab)):
                    rows = stage[slot, which, pl.ds(pl.multiple_of(r * 16, 16), 16), :].astype(F32)
                    for part in range(2):
                        base = (c * chunk + r * 16 + part * SUB) * n_col
                        for j in range(n_col):
                            tab[pl.ds(base + j, SUB, stride=n_col), :] = rows[part * SUB:(part + 1) * SUB, j * LANE:(j + 1) * LANE]

    s0 = start_ref[e]
    n = cnt_ref[e]
    unroll = 16

    @pl.loop(0, pl.cdiv(n, unroll))
    def _(b):
        first = b * unroll
        for i in range(unroll):
            row = tok_ref[s0 + first + i]
            gate = gate_ref[s0 + first + i]
            dst = pl.ds(first + i, SUB, stride=pitch)
            xtile[dst, :] = xtab[pl.ds(row, SUB), :]
            drow = dtab[pl.ds(row, SUB), :]
            gtile[dst, :] = drow * gate
            if own:
                dtile[dst, :] = drow

    tiles = (xtile, gtile, dtile) if own else (xtile, gtile)

    @pl.loop(0, cap // 16)
    def _(r):
        pos = lax.broadcasted_iota(jnp.int32, (16, LANE), 0) + r * 16
        keep = pos < n
        for tile, out in zip(tiles, outs):
            view = tile.at[pl.ds(pl.multiple_of(r * 16, 16), (n_col - 1) * pitch + 16), :]
            for j in range(n_col):
                both = jnp.where(keep, view[j * pitch:j * pitch + 16, :], 0.0).astype(BF)
                out[0, 0, pl.ds(pl.multiple_of(r * 16, 16), 16), j * LANE:(j + 1) * LANE] = both


def gather_call(plane, bufs, starts, counts, toks, gates, x_loc, d_loc, n_src, cap, own):
    n_local = starts.shape[0]
    tok_dev, width = x_loc.shape
    n_col = width // LANE
    chunk = min(512, tok_dev)
    smem = pl.BlockSpec(memory_space=pltpu.SMEM)
    anyspec = pl.BlockSpec(memory_space=pl.ANY)
    n_buf = 3 if own else 2
    table = pltpu.VMEM((tok_dev * n_col + SUB, LANE), F32)
    tile = pltpu.VMEM((SUB * pitch_for(cap), LANE), F32)
    return pl.pallas_call(
        functools.partial(gather_kernel, own, cap, chunk),
        grid=(n_local,),
        in_specs=[smem, smem, smem, smem, anyspec, anyspec] + [anyspec] * len(bufs),
        out_specs=[pl.BlockSpec((1, 1, cap, width), lambda e: (e, plane, 0, 0)) for _ in range(n_buf)],
        out_shape=[jax.ShapeDtypeStruct((n_local, n_src if i < 2 else n_src // 2, cap, width), BF) for i in range(n_buf)],
        scratch_shapes=[
            table,
            table,
            tile,
            tile,
            tile if own else pltpu.VMEM((SUB, LANE), F32),
            pltpu.VMEM((2, 2, chunk, width), BF),
            pltpu.SemaphoreType.DMA((2, 2)),
        ],
        input_output_aliases={6 + i: i for i in range(len(bufs))},
        compiler_params=pltpu.CompilerParams(vmem_limit_bytes=VMEM_LIMIT),
        name="gather_own" if own else "gather_other",
        cost_estimate=pl.CostEstimate(flops=30_000_000_000, bytes_accessed=60_000_000, transcendentals=0),
    )(starts, counts, toks, gates, x_loc, d_loc, *bufs)


def _dot(a, b):
    return jnp.dot(a, b, preferred_element_type=F32)


def _dot_t(a, b):
    return lax.dot_general(a, b, (((1,), (1,)), ((), ())), preferred_element_type=F32)


def _dot_tn(a, b):
    return lax.dot_general(a, b, (((0,), (0,)), ((), ())), preferred_element_type=F32)


def expert_kernel(own, add, n_dst, cap, base, place_ref, xs, gs, *rest):
    if own:
        ds, rest = rest[0], rest[1:]
    w_mine, w_far, rest = rest[:3], rest[3:6], rest[6:]
    if add:
        dw_in, rest = rest[:3], rest[3:]
    if own:
        dx_outs, dg_outs, rest = rest[-7 - 2 * n_dst:-7 - n_dst], rest[-7 - n_dst:-7], rest[-7:]
    dw_outs = rest[-7:-4]
    wbuf, wsem, a_scr, dh_scr = rest[-4:]
    n_own = n_dst * cap
    rows_all, width = xs.shape[1], xs.shape[2]
    ff = wbuf.shape[3]
    mine = width // 2
    half = place_ref[0]
    lo = (mine // LANE) * LANE
    wide = width - lo
    off = mine - lo
    e, n_grp = pl.program_id(0), pl.num_programs(0)
    slot = lax.rem(e, 2)

    def weights(step, at):
        copies = []
        for k in range(3):
            here = pl.ds(pl.multiple_of(half * mine, mine), mine)
            there = pl.ds(pl.multiple_of((1 - half) * mine, mine), mine)
            copies.append(pltpu.make_async_copy(w_mine[k].at[base + step], wbuf.at[at, k, here, :], wsem.at[at, k, 0]))
            copies.append(pltpu.make_async_copy(w_far[k].at[step], wbuf.at[at, k, there, :], wsem.at[at, k, 1]))
        return copies

    @pl.when(e == 0)
    def _():
        for cp in weights(0, 0):
            cp.start()

    @pl.when(e + 1 < n_grp)
    def _():
        for cp in weights(e + 1, 1 - slot):
            cp.start()

    for cp in weights(e, slot):
        cp.wait()
    w1, w3, w2 = wbuf.at[slot, 0], wbuf.at[slot, 1], wbuf.at[slot, 2]

    for blk in range(rows_all // n_own):
        rows = slice(blk * n_own, (blk + 1) * n_own)
        x = xs[0, rows, :]
        h1 = _dot(x, w1[...])
        h3 = _dot(x, w3[...])
        da = _dot(gs[0, rows, :], w2[...])
        sig = jax.nn.sigmoid(h1)
        silu = h1 * sig
        a_scr[rows, :] = (silu * h3).astype(BF)
        dh_scr[rows, :ff] = (da * h3 * sig * (1.0 + h1 * (1.0 - sig))).astype(BF)
        dh_scr[rows, ff:] = (da * silu).astype(BF)
        if own and blk == 0:
            dx = _dot_t(dh_scr[rows, :ff], w1[...]) + _dot_t(dh_scr[rows, ff:], w3[...])
            dxb = dx.astype(BF)
            for s in range(n_dst):
                dx_outs[s][0] = dxb[s * cap:(s + 1) * cap, :]
            prod = _dot_t(a_scr[rows, :], w2[...]) * ds[0].astype(F32)
            part = prod[:, :LANE]
            for j in range(1, width // LANE):
                part = part + prod[:, j * LANE:(j + 1) * LANE]
            dgate = [jnp.sum(part[r * LANE:(r + 1) * LANE, :].T, axis=0, keepdims=True) for r in range(n_own // LANE)]
            dgate = jnp.concatenate(dgate, axis=1)
            for s in range(n_dst):
                dg_outs[s][0, :, :cap] = dgate[:, s * cap:(s + 1) * cap]
    start = pl.multiple_of(half * lo, LANE)
    xh = xs[0, :, pl.ds(start, wide)]
    gh = gs[0, :, pl.ds(start, wide)]
    dw13 = _dot_tn(xh, dh_scr[...])
    dw2 = _dot_tn(gh, a_scr[...])

    def write(first):
        keep = slice(first, first + mine)
        for out, val, k in zip(dw_outs, (dw13[keep, :ff], dw2[keep, :], dw13[keep, ff:]), range(3)):
            out[0] = val + dw_in[k][0] if add else val

    @pl.when(half == 0)
    def _():
        write(0)

    @pl.when(half != 0)
    def _():
        write(off)


def expert_call(rows, place, xs, gs, ds, w_mine, w_far, base, bufs):
    n_grp, mine, ff = w_far[0].shape
    n_local, n_src, cap, width = xs.shape
    n_dst = ds.shape[1]
    own, add = rows != "other", rows == "other"
    n_rows = n_src * cap if rows == "all" else n_dst * cap
    xs = xs.reshape(n_local, n_src * cap, width)
    gs = gs.reshape(n_local, n_src * cap, width)
    ds = ds.reshape(n_local, n_dst * cap, width)
    at = lambda e: (e + base, 0, 0)
    loc = lambda e: (e, 0, 0)
    src = lambda e: (e + base, 1 if add else 0, 0)
    anyspec = pl.BlockSpec(memory_space=pl.ANY)
    args = [place, xs, gs] + ([ds] if own else []) + list(w_mine) + list(w_far)
    in_specs = [pl.BlockSpec(memory_space=pltpu.SMEM)] + [pl.BlockSpec((1, n_rows, width), src)] * 2
    in_specs += [pl.BlockSpec((1, n_dst * cap, width), at)] * own + [anyspec] * 6
    n_in = len(args)
    if bufs is not None:
        args += list(bufs)
        in_specs += [pl.BlockSpec((1, mine, ff), at) if add else anyspec] * 3
    out_specs, out_shape = [], []
    if own:
        line = pl.cdiv(cap, LANE) * LANE
        out_specs += [pl.BlockSpec((1, cap, width), loc)] * n_dst + [pl.BlockSpec((1, 1, line), loc)] * n_dst
        out_shape += [jax.ShapeDtypeStruct((n_grp, cap, width), BF)] * n_dst + [jax.ShapeDtypeStruct((n_grp, 1, line), F32)] * n_dst
    n_out = len(out_shape)
    out_specs += [pl.BlockSpec((1, mine, ff), at)] * 3
    out_shape += [jax.ShapeDtypeStruct((n_local, mine, ff), F32)] * 3
    units = {"all": 3 * n_src + 3 * n_dst + 3 * n_src // 2, "own": 6 * n_dst + 3 * n_dst // 2, "other": 3 * n_dst + 3 * n_dst // 2}[rows]
    outs = pl.pallas_call(
        functools.partial(expert_kernel, own, add, n_dst, cap, base),
        grid=(n_grp,),
        in_specs=in_specs,
        out_specs=out_specs,
        out_shape=out_shape,
        scratch_shapes=[
            pltpu.VMEM((2, 3, width, ff), BF),
            pltpu.SemaphoreType.DMA((2, 3, 2)),
            pltpu.VMEM((n_rows, ff), BF),
            pltpu.VMEM((n_rows, 2 * ff), BF),
        ],
        input_output_aliases={} if bufs is None else {n_in + i: n_out + i for i in range(3)},
        compiler_params=pltpu.CompilerParams(vmem_limit_bytes=VMEM_LIMIT),
        cost_estimate=pl.CostEstimate(flops=2 * n_grp * width * ff * units * cap, bytes_accessed=n_grp * 9_000_000, transcendentals=n_grp * n_rows * ff),
    )(*args)
    return (outs[:n_dst], outs[n_dst:n_out], outs[n_out:]) if own else outs


def combine_kernel(n_ep, base, first, last, n_rows, *refs):
    place_ref, start_ref, cnt_ref, asg_ref = refs[:4]
    rows_hbm, dg_hbm, rest = refs[4:4 + n_rows], refs[4 + n_rows:4 + 2 * n_rows], refs[4 + 2 * n_rows:]
    if not first:
        acc_in, rest = rest[0], rest[1:]
    if last:
        shared_ref, rest = rest[0], rest[1:]
        dx_out, dg_out, rest = rest[0], rest[1], rest[2:]
    else:
        acc_out, rest = rest[0], rest[1:]
    acc, tile, buf, dg_buf, sem, acc_sem = rest
    n_grp, cap, width = rows_hbm[0].shape
    n_col = width // LANE
    pitch = pitch_for(cap)
    n_exp = start_ref.shape[0]
    n_local = n_exp // n_ep
    tok_rows = acc.shape[0]
    per = n_rows // n_ep * n_grp
    unroll = 16

    def fetch(i, slot, go):
        for k in range(n_rows):
            @pl.when(lax.div(i, n_grp) == k)
            def _():
                for c, (src, dst) in enumerate(((rows_hbm[k], buf), (dg_hbm[k], dg_buf))):
                    cp = pltpu.make_async_copy(src.at[lax.rem(i, n_grp)], dst.at[slot], sem.at[slot, c])
                    cp.start() if go else cp.wait()

    fetch(0, 0, True)
    if first:
        @pl.loop(0, tok_rows // 64)
        def _(r):
            acc[pl.ds(pl.multiple_of(r * 64, 64), 64), :] = jnp.zeros((64, LANE), F32)
    else:
        pltpu.make_async_copy(acc_in, acc, acc_sem).start()
        pltpu.make_async_copy(acc_in, acc, acc_sem).wait()
    tile[n_col * pitch:, :] = jnp.zeros((tile.shape[0] - n_col * pitch, LANE), F32)
    code = jnp.where(
        lax.broadcasted_iota(jnp.int32, (SUB, LANE), 0) == n_col,
        lax.broadcasted_iota(jnp.int32, (SUB, LANE), 1),
        -1,
    )

    @pl.loop(0, n_rows * n_grp)
    def _(i):
        slot = lax.rem(i, 2)

        @pl.when(i + 1 < n_rows * n_grp)
        def _():
            fetch(i + 1, 1 - slot, True)

        fetch(i, slot, False)
        e = jnp.bitwise_xor(place_ref[1], lax.div(i, per)) * n_local + base + lax.rem(i, per)
        blocks = pl.cdiv(cnt_ref[e], unroll)

        @pl.loop(0, blocks)
        def _(r):
            view = tile.at[pl.ds(pl.multiple_of(r * 16, 16), (n_col - 1) * pitch + 16), :]
            for j in range(n_col):
                v = buf[slot, pl.ds(pl.multiple_of(r * 16, 16), 16), j * LANE:(j + 1) * LANE].astype(F32)
                view[j * pitch:j * pitch + 16, :] = v

        s0 = start_ref[e]

        @pl.loop(0, blocks)
        def _(b):
            pos = b * unroll
            for u in range(unroll):
                a = asg_ref[s0 + pos + u]
                row = tile[pl.ds(pos + u, SUB, stride=pitch), :]
                row = jnp.where(code == (a & (SUB - 1)), dg_buf[slot, 0, pos + u], row)
                dst = pl.ds(pl.multiple_of(a & -SUB, SUB), SUB)
                acc[dst, :] = acc[dst, :] + row

    if last:
        @pl.loop(0, tok_rows // (16 * SUB))
        def _(r):
            rows = pl.ds(pl.multiple_of(r * 16, 16), 16)
            both = []
            for j in range(n_col + 1):
                lo = acc[pl.ds(r * 16 * SUB + j, SUB, stride=SUB), :]
                hi = acc[pl.ds(r * 16 * SUB + SUB * SUB + j, SUB, stride=SUB), :]
                both.append(jnp.concatenate([lo, hi], axis=0))
            for j in range(n_col):
                col = slice(j * LANE, (j + 1) * LANE)
                dx_out[rows, col] = (both[j] + shared_ref[rows, col].astype(F32)).astype(BF)
            dg_out[rows, :] = both[n_col]
    else:
        pltpu.make_async_copy(acc, acc_out, acc_sem).start()
        pltpu.make_async_copy(acc, acc_out, acc_sem).wait()


def combine_call(place, starts, counts, asg, dg, rows, base, acc, shared, n_ep, tok_dev):
    n_rows = len(rows)
    first, last = acc is None, shared is not None
    _, cap, width = rows[0].shape
    smem = pl.BlockSpec(memory_space=pltpu.SMEM)
    anyspec = pl.BlockSpec(memory_space=pl.ANY)
    vmem = pl.BlockSpec(memory_space=pltpu.VMEM)
    args = [place, starts, counts, asg, *rows, *dg]
    in_specs = [smem] * 4 + [anyspec] * (2 * n_rows)
    if not first:
        args.append(acc)
        in_specs.append(anyspec)
    if last:
        args.append(shared)
        in_specs.append(vmem)
        out_shape = [jax.ShapeDtypeStruct((tok_dev, width), BF), jax.ShapeDtypeStruct((tok_dev, LANE), F32)]
        out_specs = [vmem, vmem]
    else:
        out_shape = jax.ShapeDtypeStruct((tok_dev * SUB, LANE), F32)
        out_specs = anyspec
    return pl.pallas_call(
        functools.partial(combine_kernel, n_ep, base, first, last, n_rows),
        in_specs=in_specs,
        out_specs=out_specs,
        out_shape=out_shape,
        scratch_shapes=[
            pltpu.VMEM((tok_dev * SUB, LANE), F32),
            pltpu.VMEM((SUB * pitch_for(cap), LANE), F32),
            pltpu.VMEM((2, cap, width), BF),
            pltpu.SMEM((2, 1, dg[0].shape[2]), F32),
            pltpu.SemaphoreType.DMA((2, 2)),
            pltpu.SemaphoreType.DMA,
        ],
        input_output_aliases={} if first or last else {4 + 2 * n_rows: 0},
        compiler_params=pltpu.CompilerParams(vmem_limit_bytes=VMEM_LIMIT),
        name="combine",
        cost_estimate=pl.CostEstimate(flops=n_rows * 3_000_000_000, bytes_accessed=n_rows * 3_000_000, transcendentals=0),
    )(*args)


def sort_assignments(ids_dev, gate_dev, n_exp, cap):
    n_assign = ids_dev.size
    key = ids_dev.reshape(-1) * n_assign + jnp.arange(n_assign, dtype=jnp.int32)
    key, gates = lax.sort((key, gate_dev.reshape(-1)), num_keys=1)
    edges = jnp.arange(n_exp + 1, dtype=jnp.int32) * n_assign
    starts = jnp.sum((key[None, :] < edges[:, None]).astype(jnp.int32), axis=1)
    counts = jnp.minimum(starts[1:] - starts[:-1], cap)
    pad = 2 * LANE
    asg = jnp.pad(key & (n_assign - 1), (0, pad))
    return asg, jnp.pad(gates, (0, pad)), starts[:-1], counts


def shared_backward(x_rows, g_rows, w_a, w_b, w_c):
    h_one = _dot(x_rows, w_a)
    h_three = _dot(x_rows, w_c)
    sig_one = jax.nn.sigmoid(h_one)
    silu_one = h_one * sig_one
    act_rows = (silu_one * h_three).astype(BF)
    d_act = _dot_t(g_rows, w_b)
    dh_one = (d_act * h_three * sig_one * (1.0 + h_one * (1.0 - sig_one))).astype(BF)
    dh_three = (d_act * silu_one).astype(BF)
    dx_rows = (_dot_t(dh_one, w_a) + _dot_t(dh_three, w_c)).astype(BF)
    return dx_rows, _dot_tn(x_rows, dh_one), _dot_tn(act_rows, g_rows), _dot_tn(x_rows, dh_three)


def solution(mesh):
    ep_size = mesh.shape["ep"]
    rows_size = mesh.shape["fsdp"]
    tok_spec = P(("fsdp", "ep"), None)
    in_specs = (tok_spec, tok_spec, tok_spec, tok_spec, P("ep", "fsdp", None), P("ep", None, "fsdp"), P("ep", "fsdp", None), P("fsdp", None), P(None, "fsdp"), P("fsdp", None))
    out_specs = (tok_spec, tok_spec, P("ep", "fsdp", None), P("ep", None, "fsdp"), P("ep", "fsdp", None), P("fsdp", None), P(None, "fsdp"), P("fsdp", None))
    cuts = (0, 4, 6, 7, 8)
    kernels = ["gather_0", "gather_1", "gather_2", "gather_3", "gather_4", "gather_5", "own_0", "own_1", "gather_6", "gather_7", "all_2", "other_0", "other_1"]
    kernels += ["all_3", "all_4", "all_5", "combine_0", "all_6", "combine_1", "all_7", "combine_2", "combine_3"]

    def swap_row(v):
        return lax.ppermute(v, "fsdp", [(i, rows_size - 1 - i) for i in range(rows_size)])

    def swap_ep(v, k):
        return lax.ppermute(v, "ep", [(i, i ^ k) for i in range(ep_size)])

    def device_step(x_loc, dy_loc, ids_loc, gate_loc, w_one, w_two, w_three, ws_one, ws_two, ws_three):
        tok_dev, top_k = ids_loc.shape
        assert top_k == SUB
        n_local = w_one.shape[0]
        n_exp = n_local * ep_size
        n_src = ep_size * rows_size
        n_col = x_loc.shape[1] // LANE
        cap = capacity_for(tok_dev, top_k, n_exp)
        n_grp = n_local // N_GROUP
        me, row = lax.axis_index("ep"), lax.axis_index("fsdp")
        place = jnp.stack([row, me]).astype(jnp.int32)

        near = (x_loc, dy_loc)
        far = tuple(swap_row(v) for v in near)
        near_x = tuple(swap_ep(v, 2) for v in near)
        near_c = tuple(swap_ep(v, 1) for v in near)

        w_mine = (w_one, w_three, jnp.swapaxes(w_two, 1, 2))
        w_far = []
        for g in range(N_GROUP):
            w_far.append(tuple(swap_row(w[g * n_grp:(g + 1) * n_grp]) for w in w_mine))

        ws_one_full = lax.all_gather(ws_one, "fsdp", axis=0, tiled=True)
        ws_three_full = lax.all_gather(ws_three, "fsdp", axis=0, tiled=True)
        ws_two_full = lax.all_gather(ws_two, "fsdp", axis=1, tiled=True)
        shared = shared_backward(x_loc, dy_loc, ws_one_full, ws_two_full, ws_three_full)
        dws_one = lax.psum(lax.psum_scatter(shared[1], "fsdp", scatter_dimension=0, tiled=True), "ep")
        dws_two = lax.psum(lax.psum_scatter(shared[2], "fsdp", scatter_dimension=1, tiled=True), "ep")
        dws_three = lax.psum(lax.psum_scatter(shared[3], "fsdp", scatter_dimension=0, tiled=True), "ep")

        ids_loc, gate_loc, shared = lax.optimization_barrier((ids_loc, gate_loc, shared))
        asg, gates, starts, counts = sort_assignments(ids_loc, gate_loc, n_exp, cap)
        n_list = asg.shape[0]
        meta = jnp.concatenate([(asg // top_k) * n_col, starts, counts])
        meta_all = lax.all_gather(meta, ("fsdp", "ep"), axis=0)
        gates_all = lax.all_gather(gates, ("fsdp", "ep"), axis=0)

        def gather(plane, bufs, x_src, dy_src):
            own = plane < ep_size
            if plane == 0:
                meta_s, gates_s = meta, gates
            else:
                src = jnp.bitwise_xor(me, plane % ep_size) + ep_size * (row if own else rows_size - 1 - row)
                meta_s = lax.dynamic_index_in_dim(meta_all, src, 0, keepdims=False)
                gates_s = lax.dynamic_index_in_dim(gates_all, src, 0, keepdims=False)
            starts_s = lax.dynamic_slice(meta_s, (n_list + me * n_local,), (n_local,))
            counts_s = lax.dynamic_slice(meta_s, (n_list + n_exp + me * n_local,), (n_local,))
            take = tuple(bufs) if own else tuple(bufs[:2])
            new = gather_call(plane, take, starts_s, counts_s, meta_s[:n_list], gates_s, x_src, dy_src, n_src, cap, own)
            return tuple(new) + tuple(bufs[len(new):])

        near_xc = tuple(swap_ep(v, 1) for v in near_x)
        far_x = tuple(swap_ep(v, 2) for v in far)
        far_c = tuple(swap_ep(v, 1) for v in far)
        far_xc = tuple(swap_ep(v, 1) for v in far_x)
        srcs = (near, near_c, near_x, near_xc, far, far_c, far_x, far_xc)
        bufs, grads = (), None
        back_rows, part_dg = [None] * N_GROUP, [None] * N_GROUP
        acc = None
        for name in kernels:
            kind, i = name.split("_")
            i = int(i)
            if kind == "gather":
                bufs = gather(i, bufs, *srcs[i])
                continue
            if kind == "combine":
                lo, hi = cuts[i], cuts[i + 1]
                dg = [part_dg[g][k] for k in range(ep_size) for g in range(lo, hi)]
                rows = [back_rows[g][k] for k in range(ep_size) for g in range(lo, hi)]
                final = shared[0] if hi == N_GROUP else None
                acc = combine_call(place, starts, counts, asg, dg, rows, lo * n_grp, acc, final, ep_size, tok_dev)
                continue
            xs, gs, ds = bufs
            out = expert_call(kind, place, xs, gs, ds, w_mine, w_far[i], i * n_grp, grads)
            if kind == "other":
                grads = out
                continue
            dx_g, dg_g, grads = out
            part_dg[i] = [dg_g[0]] + [swap_ep(dg_g[k], k) for k in range(1, ep_size)]
            back_rows[i] = [dx_g[0]] + [swap_ep(dx_g[k], k) for k in range(1, ep_size)]
        dx_loc, dg_tok = acc
        dw_one, dw_two, dw_three = grads
        return dx_loc, dg_tok[:, :top_k], dw_one, jnp.swapaxes(dw_two, 1, 2), dw_three, dws_one, dws_two, dws_three


    return jax.shard_map(device_step, mesh=mesh, in_specs=in_specs, out_specs=out_specs, check_vma=False)
```
